32 devices in a mesh: wide: 8 (over y, x, core), narrow: 4 (over z).
Axes of the slice: x: 2, y: 2, z: 4, core: 2. Of those that a mesh axis runs over, the one named last changes fastest.
Arguments:
- local_slopes: float32 [32, 512, 128], P(('wide', 'narrow')), may hold values from -0.25 to 0.25
- global_slopes: float32 [32, 512, 1024], P(('wide', 'narrow')), may hold values from -0.25 to 0.25
- residuals: float32 [32, 512], P(('wide', 'narrow')), may hold values from -6 to 6
- weights: float32 [32, 512], P(('wide', 'narrow')), may hold values from 0.1 to 10
- track_slot_count: int32 [32], P(('wide', 'narrow')), may hold values from 64 to 512
- windows: int32 [32], P(('wide', 'narrow')), may hold values from 0 to 3
Outputs:
- normal_matrix: float32 [4, 1024, 1024], P(None, 'narrow', 'wide')
- normal_rhs: float32 [4, 1024], P(None, 'narrow')
The draws below stay inside these ranges and needn't reach their ends.
All inputs are finite; a program needn't handle non-finite values.
Results may differ from the reference program's by a relative error of at most 0.0003.
Values sent between devices are 32-bit elements; how exact they have to be, the bound alone decides.
A program may use at most 64 MiB of HBM per device.

```python
import math
import jax
import jax.numpy as jnp
from jax import lax

WINDOW_PARAMS = 1024
LOCAL_PARAMS = 128
MEASURE_SLOTS = 512
NWIN = 4
TRACK_BUNDLES = 32


def set_ends(drawn, own_key, low, top_value):
    index_at = [jax.random.randint(jax.random.fold_in(own_key, axis), (), 0, length) for axis, length in enumerate(drawn.shape)]
    main_axis = drawn.shape.index(max(drawn.shape))
    next_to = index_at[:main_axis] + [(index_at[main_axis] + 1) % drawn.shape[main_axis]] + index_at[main_axis + 1:]
    return drawn.at[tuple(index_at)].set(low).at[tuple(next_to)].set(top_value)


def levels(stream_key, extent, shards, least, top_value):
    level = 1.0
    for dim, shards_of in shards:
        draws = jax.random.uniform(jax.random.fold_in(jax.random.fold_in(stream_key, 6), dim), (shards_of,), jnp.float32, least / len(shards), top_value / len(shards))
        level = level * jnp.repeat(jnp.exp(draws), extent[dim] // shards_of).reshape((-1,) + (1,) * (len(extent) - 1 - dim))
    return level


def bell_draw(key, dims, scale, most, shards=(), held_as=jnp.bfloat16):
    entries = scale * jax.random.normal(key, dims, jnp.float32)
    if shards:
        entries = entries * levels(key, dims, shards, -0.22, 0.18)
    return jnp.clip(entries, -most, most).astype(held_as)


def setup_inputs(seed: int = 0) -> dict:
    arg_keys = jax.random.split(jax.random.key(seed), 7)
    local_slopes = bell_draw(arg_keys[0], (TRACK_BUNDLES, MEASURE_SLOTS, LOCAL_PARAMS), MEASURE_SLOTS ** -0.5, 0.25, ((0, 32),), jnp.float32)
    global_slopes = bell_draw(arg_keys[1], (TRACK_BUNDLES, MEASURE_SLOTS, WINDOW_PARAMS), MEASURE_SLOTS ** -0.5, 0.25, ((0, 32),), jnp.float32)
    residuals = bell_draw(arg_keys[2], (TRACK_BUNDLES, MEASURE_SLOTS), 1.0, 6.0, ((0, 32),), jnp.float32)
    weights = jnp.clip(jnp.exp(math.log(10.0) - 4.6051702 * jax.random.uniform(arg_keys[3], (TRACK_BUNDLES, MEASURE_SLOTS), jnp.float32) ** levels(arg_keys[3], (TRACK_BUNDLES, MEASURE_SLOTS), ((0, 32),), -0.2, 0.2)), 0.1, 10.0)
    track_slot_count = set_ends(jax.random.randint(arg_keys[4], (TRACK_BUNDLES,), MEASURE_SLOTS // 8, MEASURE_SLOTS + 1), jax.random.fold_in(arg_keys[4], 1), MEASURE_SLOTS // 8, MEASURE_SLOTS).astype(jnp.int32)
    windows = set_ends(jax.random.randint(arg_keys[5], (TRACK_BUNDLES,), 0, NWIN), jax.random.fold_in(arg_keys[5], 1), 0, NWIN - 1).astype(jnp.int32)
    return {"local_slopes": local_slopes, "global_slopes": global_slopes, "residuals": residuals, "weights": weights, "track_slot_count": track_slot_count, "windows": windows}


def tdot(left, right):
    return lax.dot_general(left.astype(jnp.float32), right.astype(jnp.float32), (((0,), (0,)), ((), ())), precision=lax.Precision.HIGHEST, preferred_element_type=jnp.float32)

def reference(local_slopes, global_slopes, residuals, weights, track_slot_count, windows):
    slot_entries = jnp.arange(MEASURE_SLOTS, dtype=jnp.int32)

    def one_bundle(carry, items):
        matrix, rhs = carry
        local_b, global_b, resid_b, weight_b, count_b, window_b = items
        live = jnp.where(slot_entries < count_b, weight_b, jnp.float32(0.0))
        wl = local_b * live[:, None]
        wg = global_b * live[:, None]
        curv = tdot(wl, local_b) + jnp.eye(LOCAL_PARAMS, dtype=jnp.float32)
        coupling = tdot(wl, global_b)
        lr = tdot(wl, resid_b[:, None])
        gram = tdot(wg, global_b)
        gr = tdot(wg, resid_b[:, None])[:, 0]
        factor = jnp.linalg.cholesky(curv)
        solved = jax.scipy.linalg.cho_solve((factor, True), jnp.concatenate([coupling, lr], axis=1))
        schur = gram - tdot(coupling, solved[:, :WINDOW_PARAMS])
        srhs = gr - tdot(coupling, solved[:, WINDOW_PARAMS:])[:, 0]
        picks = (jnp.arange(NWIN, dtype=jnp.int32) == window_b).astype(jnp.float32)
        matrix = matrix + picks[:, None, None] * schur[None]
        rhs = rhs + picks[:, None] * srhs[None]
        return ((matrix, rhs), None)
    start = (jnp.zeros((NWIN, WINDOW_PARAMS, WINDOW_PARAMS), jnp.float32), jnp.zeros((NWIN, WINDOW_PARAMS), jnp.float32))
    (matrix, rhs), _ = lax.scan(one_bundle, start, (local_slopes, global_slopes, residuals, weights, track_slot_count, windows))
    return (matrix, rhs)
```

```python
import functools
import jax
import jax.numpy as jnp
from jax import lax
from jax.experimental import pallas as pl
from jax.experimental.pallas import tpu as pltpu
from jax.sharding import PartitionSpec as P

WINDOW_PARAMS = 1024
NWIN = 4
LANES = 128
CHUNK = 64
AHEAD = 3
LAG = 2
MESH = pl.DeviceIdType.MESH
HIGHEST = lax.Precision.HIGHEST
HIGH = lax.Precision.HIGH


def tdot(left, right, precision=HIGHEST):
    return lax.dot_general(
        left,
        right,
        (((0,), (0,)), ((), ())),
        precision=precision,
        preferred_element_type=jnp.float32,
    )


def invert_kernel(c_ref, out_ref):
    size = c_ref.shape[0]
    sub = lax.broadcasted_iota(jnp.int32, (size, 1), 0)
    lane = lax.broadcasted_iota(jnp.int32, (1, size), 1)
    c = c_ref[...]
    for k in range(0, size, 2):
        r0, r1 = c[k:k + 1, :], c[k + 1:k + 2, :]
        c0, c1 = c[:, k:k + 1], c[:, k + 1:k + 2]
        a, b, d = r0[:, k:k + 1], r0[:, k + 1:k + 2], r1[:, k + 1:k + 2]
        b_low = r1[:, k:k + 1]
        inv = 1.0 / (a * d - b * b_low)
        here, after = lane == k, lane == k + 1
        r0 = jnp.where(here, 1.0, jnp.where(after, 0.0, r0))
        r1 = jnp.where(after, 1.0, jnp.where(here, 0.0, r1))
        p0 = (d * inv) * r0 - (b * inv) * r1
        p1 = (a * inv) * r1 - (b_low * inv) * r0
        f0 = jnp.where(sub == k, -1.0, jnp.where(sub == k + 1, 0.0, c0))
        f1 = jnp.where(sub == k + 1, -1.0, jnp.where(sub == k, 0.0, c1))
        pivot = (sub == k) | (sub == k + 1) | here | after
        c = jnp.where(pivot, 0.0, c) - f0 * p0 - f1 * p1
    out_ref[...] = c


def invert(c):
    return pl.pallas_call(
        invert_kernel,
        out_shape=jax.ShapeDtypeStruct(c.shape, jnp.float32),
        in_specs=[pl.BlockSpec(memory_space=pltpu.VMEM)],
        out_specs=pl.BlockSpec(memory_space=pltpu.VMEM),
        name="invert",
    )(c)


def spread_kernel(nq, nz, s_ref, small_ref, out_ref, rhs_ref,
                  recv, small, part, from_lo, from_hi, rsum, rrecv,
                  own_sem, send_sem, recv_sem, small_send, small_recv,
                  z_send, lo_sem, hi_sem, r_send, r_recv):
    q = lax.axis_index("wide")
    z = lax.axis_index("narrow")
    chunks = recv.shape[1]
    rows = chunks // nz

    def peer(step):
        return lax.rem(q + step, nq)

    barrier = pltpu.get_barrier_semaphore()
    for step in range(1, nq):
        pl.semaphore_signal(barrier, inc=1, device_id=(peer(step), z), device_id_type=MESH)
    for step in range(1, nz):
        pl.semaphore_signal(barrier, inc=1, device_id=(q, lax.rem(z + step, nz)), device_id_type=MESH)
    pl.semaphore_wait(barrier, nq - 1 + nz - 1)

    def piece(t, col):
        row = lax.rem(t, nz) * (rows * CHUNK) + (t // nz) * CHUNK
        return s_ref.at[pl.ds(pl.multiple_of(row, CHUNK), CHUNK), pl.ds(pl.multiple_of(col * LANES, LANES), LANES)]

    def plane_copy(t, step):
        return pltpu.make_async_remote_copy(
            src_ref=piece(t, peer(step)), dst_ref=recv.at[nq - step, t],
            send_sem=send_sem.at[step, t], recv_sem=recv_sem.at[nq - step, t],
            device_id=(peer(step), z), device_id_type=MESH)

    def own_copy(t):
        return pltpu.make_async_copy(piece(t, q), recv.at[0, t], own_sem.at[t])

    def small_copy(step):
        return pltpu.make_async_remote_copy(
            src_ref=small_ref, dst_ref=small.at[nq - step],
            send_sem=small_send.at[step], recv_sem=small_recv.at[nq - step],
            device_id=(peer(step), z), device_id_type=MESH)

    def up_copy(t):
        return pltpu.make_async_remote_copy(
            src_ref=part.at[t], dst_ref=from_lo.at[t], send_sem=z_send.at[t], recv_sem=lo_sem.at[t],
            device_id=(q, lax.min(z + 1, nz - 1)), device_id_type=MESH)

    def down_copy(t):
        return pltpu.make_async_remote_copy(
            src_ref=part.at[t], dst_ref=from_hi.at[t], send_sem=z_send.at[t], recv_sem=hi_sem.at[t],
            device_id=(q, lax.max(z - 1, 0)), device_id_type=MESH)

    def rhs_copy(step):
        return pltpu.make_async_remote_copy(
            src_ref=rsum, dst_ref=rrecv.at[nz - step],
            send_sem=r_send.at[step], recv_sem=r_recv.at[nz - step],
            device_id=(q, lax.rem(z + step, nz)), device_id_type=MESH)

    order = sorted(range(1, nq), key=lambda step: -min(step, nq - step))

    def send_chunk(t):
        for step in order:
            plane_copy(t, step).start()
        own_copy(t).start()

    for step in order:
        small_copy(step).start()
    for t in range(AHEAD):
        send_chunk(t)
    small[0] = small_ref[...]
    for step in range(1, nq):
        small_copy(nq - step).wait_recv()
    groups = small.shape[1] // 2
    for w in range(NWIN):
        total = jnp.zeros((groups, LANES), jnp.float32)
        for s in range(nq):
            total = total + small[s, groups + w:groups + w + 1, :] * small[s, :groups, :]
        rsum[w] = total
    for step in range(1, nz):
        rhs_copy(step).start()

    def relay(t, hop):
        n = lax.rem(t, nz)
        if hop == 0:
            @pl.when((z == 0) & (n > 0))
            def _():
                up_copy(t).start()

            @pl.when((z == nz - 1) & (n < nz - 1))
            def _():
                down_copy(t).start()
        else:
            @pl.when((z == hop) & (n > z))
            def _():
                up_copy(t).wait_recv()
                part[t] = part[t] + from_lo[t]
                up_copy(t).start()

            @pl.when((z == nz - 1 - hop) & (n < z))
            def _():
                down_copy(t).wait_recv()
                part[t] = part[t] + from_hi[t]
                down_copy(t).start()

    def body(t, carry):
        @pl.when(t + AHEAD < chunks)
        def _():
            send_chunk(t + AHEAD)

        @pl.when(t < chunks)
        def _():
            own_copy(t).wait()
            for step in order:
                plane_copy(t, nq - step).wait_recv()
            for w in range(NWIN):
                total = jnp.zeros((CHUNK, LANES), jnp.float32)
                for s in range(nq):
                    total = total + small[s, groups + w:groups + w + 1, :] * recv[s, t]
                part[t, w] = total
            relay(t, 0)
        for hop in range(1, nz - 1):
            late = t - LAG * hop

            @pl.when((late >= 0) & (late < chunks))
            def _(late=late, hop=hop):
                relay(late, hop)
        return carry

    lax.fori_loop(0, chunks + LAG * (nz - 2), body, 0)

    def finish(j, carry):
        t = j * nz + z

        @pl.when(z > 0)
        def _():
            up_copy(t).wait_recv()
            part[t] = part[t] + from_lo[t]

        @pl.when(z < nz - 1)
        def _():
            down_copy(t).wait_recv()
            part[t] = part[t] + from_hi[t]
        out_ref[:, pl.ds(pl.multiple_of(j * CHUNK, CHUNK), CHUNK), :] = part[t]
        return carry

    lax.fori_loop(0, rows, finish, 0)

    for step in range(1, nz):
        rhs_copy(nz - step).wait_recv()
    total = rsum[...]
    for step in range(1, nz):
        total = total + rrecv[step]
    rhs_ref[...] = total

    for step in range(1, nq):
        small_copy(step).wait_send()
    for step in range(1, nz):
        rhs_copy(step).wait_send()

    def drain(t, carry):
        for step in range(1, nq):
            plane_copy(t, step).wait_send()

        @pl.when(lax.rem(t, nz) != z)
        def _():
            up_copy(t).wait_send()
        return carry

    lax.fori_loop(0, chunks, drain, 0)


def spread(nq, nz, schur, small):
    params = schur.shape[0]
    chunks = params // CHUNK
    groups = params // LANES
    block = pltpu.VMEM((chunks, NWIN, CHUNK, LANES), jnp.float32)
    dma = pltpu.SemaphoreType.DMA
    return pl.pallas_call(
        functools.partial(spread_kernel, nq, nz),
        out_shape=(jax.ShapeDtypeStruct((NWIN, params // nz, LANES), jnp.float32),
                   jax.ShapeDtypeStruct((NWIN, groups, LANES), jnp.float32)),
        in_specs=[pl.BlockSpec(memory_space=pl.ANY), pl.BlockSpec(memory_space=pltpu.VMEM)],
        out_specs=(pl.BlockSpec(memory_space=pltpu.VMEM), pl.BlockSpec(memory_space=pltpu.VMEM)),
        scratch_shapes=[
            pltpu.VMEM((nq, chunks, CHUNK, LANES), jnp.float32),
            pltpu.VMEM((nq, 2 * groups, LANES), jnp.float32),
            block, block, block,
            pltpu.VMEM((NWIN, groups, LANES), jnp.float32),
            pltpu.VMEM((nz, NWIN, groups, LANES), jnp.float32),
            dma((chunks,)), dma((nq, chunks)), dma((nq, chunks)), dma((nq,)), dma((nq,)),
            dma((chunks,)), dma((chunks,)), dma((chunks,)), dma((nz,)), dma((nz,)),
        ],
        compiler_params=pltpu.CompilerParams(
            collective_id=0, has_side_effects=True, vmem_limit_bytes=40 * 1024 * 1024),
        name="spread",
    )(schur, small)


def reduced_bundle(local_b, global_b, resid_b, weight_b, count):
    measure_slot, local_param = local_b.shape
    slots = jnp.arange(measure_slot, dtype=jnp.int32)
    live = jnp.where(slots < count, weight_b, jnp.float32(0.0))
    root = jnp.sqrt(live)[:, None]
    ls = local_b * root
    gs = global_b * root
    rs = resid_b[:, None] * root
    curv = tdot(ls, ls) + jnp.eye(local_param, dtype=jnp.float32)
    coupling = tdot(ls, gs)
    lr = tdot(ls, rs)
    gr = tdot(gs, rs)[:, 0]
    inverse = invert(curv)
    solved = tdot(inverse, coupling)
    solved_rhs = tdot(inverse, lr)
    schur = tdot(gs, gs, HIGH) - tdot(coupling, solved, HIGH)
    reduced = gr - tdot(coupling, solved_rhs)[:, 0]
    return schur, reduced


def on_device(local_slopes, global_slopes, residuals, weights, track_slot_count, windows):
    nq, nz = lax.axis_size("wide"), lax.axis_size("narrow")
    params = global_slopes.shape[2]
    schur, reduced = reduced_bundle(
        local_slopes[0], global_slopes[0], residuals[0], weights[0], track_slot_count[0])
    picks = (windows[0] == jnp.arange(NWIN, dtype=jnp.int32)).astype(jnp.float32)
    owned = params // nz
    z = lax.axis_index("narrow")
    if params // nq == LANES and owned % CHUNK == 0 and nz > 1:
        groups = params // LANES
        picks = jnp.pad(jnp.broadcast_to(picks[:, None], (NWIN, LANES)), ((0, groups - NWIN), (0, 0)))
        small = jnp.concatenate([reduced.reshape(groups, LANES), picks], axis=0)
        matrix, rhs = spread(nq, nz, schur, small)
        return matrix, lax.dynamic_slice_in_dim(rhs.reshape(NWIN, params), z * owned, owned, 1)
    rhs_whole = lax.psum(picks[:, None] * reduced[None], ("wide", "narrow"))
    normal_rhs = lax.dynamic_slice_in_dim(rhs_whole, z * owned, owned, 1)
    received = lax.all_to_all(schur[None], "wide", split_axis=2, concat_axis=0, tiled=True)
    all_picks = lax.all_gather(picks, "wide", axis=0)
    partial_value = jnp.einsum("bw,bij->wij", all_picks, received, precision=HIGHEST,
                               preferred_element_type=jnp.float32)
    return lax.psum_scatter(partial_value, "narrow", scatter_dimension=1, tiled=True), normal_rhs


def solution(mesh):
    in_specs = (
        P(("wide", "narrow"), None, None),
        P(("wide", "narrow"), None, None),
        P(("wide", "narrow"), None),
        P(("wide", "narrow"), None),
        P(("wide", "narrow")),
        P(("wide", "narrow")),
    )
    out_specs = (P(None, "narrow", "wide"), P(None, "narrow"))
    return jax.shard_map(
        on_device, mesh=mesh, in_specs=in_specs, out_specs=out_specs, check_vma=False
    )
```

```python
import functools
import jax
import jax.numpy as jnp
from jax import lax
from jax.experimental import pallas as pl
from jax.experimental.pallas import tpu as pltpu
from jax.sharding import PartitionSpec as P

WINDOW_PARAMS = 1024
NWIN = 4
LANES = 128
CHUNK = 64
AHEAD = 3
LAG = 2
MESH = pl.DeviceIdType.MESH
HIGHEST = lax.Precision.HIGHEST
HIGH = lax.Precision.HIGH


def tdot(left, right, precision=HIGHEST):
    return lax.dot_general(
        left,
        right,
        (((0,), (0,)), ((), ())),
        precision=precision,
        preferred_element_type=jnp.float32,
    )


def invert(c):
    size = c.shape[0]
    sub = lax.broadcasted_iota(jnp.int32, (8, size), 0)
    lane = lax.broadcasted_iota(jnp.int32, (8, size), 1)
    rows = [c[r:r + 8, :] for r in range(0, size, 8)]
    for k in range(0, size, 2):
        r, o = divmod(k, 8)
        left = [jnp.broadcast_to(x[:, k:k + 1], x.shape) for x in rows]
        right = [jnp.broadcast_to(x[:, k + 1:k + 2], x.shape) for x in rows]
        r0 = jnp.broadcast_to(rows[r][o:o + 1, :], (8, size))
        r1 = jnp.broadcast_to(rows[r][o + 1:o + 2, :], (8, size))
        a = jnp.broadcast_to(left[r][o:o + 1, :], (8, size))
        b_low = jnp.broadcast_to(left[r][o + 1:o + 2, :], (8, size))
        b = jnp.broadcast_to(right[r][o:o + 1, :], (8, size))
        d = jnp.broadcast_to(right[r][o + 1:o + 2, :], (8, size))
        inv = 1.0 / (a * d - b * b_low)
        here, after = lane == k, lane == k + 1
        r0 = jnp.where(here, 1.0, jnp.where(after, 0.0, r0))
        r1 = jnp.where(after, 1.0, jnp.where(here, 0.0, r1))
        p0 = (d * r0 - b * r1) * inv
        p1 = (a * r1 - b_low * r0) * inv
        pair = here | after
        rows = [jnp.where(pair, 0.0, x) - u * p0 - v * p1 for x, u, v in zip(rows, left, right)]
        rows[r] = jnp.where(sub == o, p0, jnp.where(sub == o + 1, p1, rows[r]))
    return jnp.concatenate(rows, axis=0)


def split(x):
    high = x.astype(jnp.bfloat16)
    return high, (x - high.astype(jnp.float32)).astype(jnp.bfloat16)


def bundle_kernel(count_ref, window_ref, local_ref, global_ref, resid_ref, weight_ref,
                  schur_ref, small_ref, high, low, u_high, u_low, x_high, x_low, gr):
    slots, params = global_ref.shape
    size = local_ref.shape[1]
    groups = params // LANES
    slot = lax.broadcasted_iota(jnp.int32, (1, slots), 1)
    root = jnp.sqrt(jnp.where(slot < count_ref[0], weight_ref[...], 0.0))
    root_col = jnp.broadcast_to(root, (LANES, slots)).T
    rs_col = jnp.broadcast_to(root * resid_ref[...], (LANES, slots)).T
    ls = local_ref[...] * root_col
    eye = (lax.broadcasted_iota(jnp.int32, (size, size), 0)
           == lax.broadcasted_iota(jnp.int32, (size, size), 1)).astype(jnp.float32)
    ls_t = ls.T
    inverse = invert(jnp.dot(ls_t, ls, precision=HIGHEST, preferred_element_type=jnp.float32) + eye)
    lr = jnp.sum(ls * rs_col, axis=0, keepdims=True)
    lr_col = jnp.broadcast_to(lr, (LANES, size)).T
    for g in range(groups):
        cols = slice(g * LANES, (g + 1) * LANES)
        gs = global_ref[:, cols] * root_col
        high[:, cols], low[:, cols] = split(gs)
        coupling = jnp.dot(ls_t, gs, precision=HIGHEST, preferred_element_type=jnp.float32)
        solved = jnp.dot(inverse, coupling, precision=HIGHEST, preferred_element_type=jnp.float32)
        u_high[:, cols], u_low[:, cols] = split(coupling)
        x_high[:, cols], x_low[:, cols] = split(solved)
        gr[g:g + 1, :] = (jnp.sum(gs * rs_col, axis=0, keepdims=True)
                          - jnp.sum(solved * lr_col, axis=0, keepdims=True))
    small_ref[:groups, :] = gr[...]
    small_ref[groups:, :] = (lax.broadcasted_iota(jnp.int32, (groups, LANES), 0)
                             == window_ref[0]).astype(jnp.float32)

    @pl.loop(0, groups)
    def _(i):
        cols = pl.ds(pl.multiple_of(i * LANES, LANES), LANES)

        def product(left, right):
            return lax.dot_general(left[:, cols], right[...], (((0,), (0,)), ((), ())),
                                   preferred_element_type=jnp.float32)

        gram = product(high, high) + (product(high, low) + product(low, high))
        taken = product(u_high, x_high) + (product(u_high, x_low) + product(u_low, x_high))
        schur_ref[cols, :] = gram - taken


def reduce_bundle(count, window, local_b, global_b, resid, weight):
    slots, params = global_b.shape
    size = local_b.shape[1]
    groups = params // LANES
    smem = pl.BlockSpec(memory_space=pltpu.SMEM)
    vmem = pl.BlockSpec(memory_space=pltpu.VMEM)
    bf16 = jnp.bfloat16
    return pl.pallas_call(
        bundle_kernel,
        out_shape=(jax.ShapeDtypeStruct((params, params), jnp.float32),
                   jax.ShapeDtypeStruct((2 * groups, LANES), jnp.float32)),
        in_specs=[smem, smem, vmem, vmem, vmem, vmem],
        out_specs=(vmem, vmem),
        scratch_shapes=[
            pltpu.VMEM((slots, params), bf16), pltpu.VMEM((slots, params), bf16),
            pltpu.VMEM((size, params), bf16), pltpu.VMEM((size, params), bf16),
            pltpu.VMEM((size, params), bf16), pltpu.VMEM((size, params), bf16),
            pltpu.VMEM((groups, LANES), jnp.float32),
        ],
        compiler_params=pltpu.CompilerParams(vmem_limit_bytes=24 * 1024 * 1024),
        name="bundle",
    )(count, window, local_b, global_b, resid, weight)


def spread_kernel(nq, nz, s_ref, small_ref, out_ref, rhs_ref,
                  recv, small, part, from_lo, from_hi, rsum, rrecv,
                  own_sem, send_sem, recv_sem, small_send, small_recv,
                  z_send, lo_sem, hi_sem, r_send, r_recv):
    q = lax.axis_index("wide")
    z = lax.axis_index("narrow")
    chunks = recv.shape[1]
    rows = chunks // nz

    def peer(step):
        return lax.rem(q + step, nq)

    barrier = pltpu.get_barrier_semaphore()
    for step in range(1, nq):
        pl.semaphore_signal(barrier, inc=1, device_id=(peer(step), z), device_id_type=MESH)
    for step in range(1, nz):
        pl.semaphore_signal(barrier, inc=1, device_id=(q, lax.rem(z + step, nz)), device_id_type=MESH)
    pl.semaphore_wait(barrier, nq - 1 + nz - 1)

    def piece(t, col):
        row = lax.rem(t, nz) * (rows * CHUNK) + (t // nz) * CHUNK
        return s_ref.at[pl.ds(pl.multiple_of(row, CHUNK), CHUNK), pl.ds(pl.multiple_of(col * LANES, LANES), LANES)]

    def plane_copy(t, step):
        return pltpu.make_async_remote_copy(
            src_ref=piece(t, peer(step)), dst_ref=recv.at[nq - step, t],
            send_sem=send_sem.at[step, t], recv_sem=recv_sem.at[nq - step, t],
            device_id=(peer(step), z), device_id_type=MESH)

    def own_copy(t):
        return pltpu.make_async_copy(piece(t, q), recv.at[0, t], own_sem.at[t])

    def small_copy(step):
        return pltpu.make_async_remote_copy(
            src_ref=small_ref, dst_ref=small.at[nq - step],
            send_sem=small_send.at[step], recv_sem=small_recv.at[nq - step],
            device_id=(peer(step), z), device_id_type=MESH)

    def up_copy(t):
        return pltpu.make_async_remote_copy(
            src_ref=part.at[t], dst_ref=from_lo.at[t], send_sem=z_send.at[t], recv_sem=lo_sem.at[t],
            device_id=(q, lax.min(z + 1, nz - 1)), device_id_type=MESH)

    def down_copy(t):
        return pltpu.make_async_remote_copy(
            src_ref=part.at[t], dst_ref=from_hi.at[t], send_sem=z_send.at[t], recv_sem=hi_sem.at[t],
            device_id=(q, lax.max(z - 1, 0)), device_id_type=MESH)

    def rhs_copy(step):
        return pltpu.make_async_remote_copy(
            src_ref=rsum, dst_ref=rrecv.at[nz - step],
            send_sem=r_send.at[step], recv_sem=r_recv.at[nz - step],
            device_id=(q, lax.rem(z + step, nz)), device_id_type=MESH)

    order = sorted(range(1, nq), key=lambda step: -min(step, nq - step))

    def send_chunk(t):
        for step in order:
            plane_copy(t, step).start()
        own_copy(t).start()

    for step in order:
        small_copy(step).start()
    for t in range(AHEAD):
        send_chunk(t)
    small[0] = small_ref[...]
    for step in range(1, nq):
        small_copy(nq - step).wait_recv()
    groups = small.shape[1] // 2
    for w in range(NWIN):
        total = jnp.zeros((groups, LANES), jnp.float32)
        for s in range(nq):
            total = total + small[s, groups + w:groups + w + 1, :] * small[s, :groups, :]
        rsum[w] = total
    for step in range(1, nz):
        rhs_copy(step).start()

    def relay(t, hop):
        n = lax.rem(t, nz)
        if hop == 0:
            @pl.when((z == 0) & (n > 0))
            def _():
                up_copy(t).start()

            @pl.when((z == nz - 1) & (n < nz - 1))
            def _():
                down_copy(t).start()
        else:
            @pl.when((z == hop) & (n > z))
            def _():
                up_copy(t).wait_recv()
                part[t] = part[t] + from_lo[t]
                up_copy(t).start()

            @pl.when((z == nz - 1 - hop) & (n < z))
            def _():
                down_copy(t).wait_recv()
                part[t] = part[t] + from_hi[t]
                down_copy(t).start()

    def body(t, carry):
        @pl.when(t + AHEAD < chunks)
        def _():
            send_chunk(t + AHEAD)

        @pl.when(t < chunks)
        def _():
            own_copy(t).wait()
            for step in order:
                plane_copy(t, nq - step).wait_recv()
            for w in range(NWIN):
                total = jnp.zeros((CHUNK, LANES), jnp.float32)
                for s in range(nq):
                    total = total + small[s, groups + w:groups + w + 1, :] * recv[s, t]
                part[t, w] = total
            relay(t, 0)
        for hop in range(1, nz - 1):
            late = t - LAG * hop

            @pl.when((late >= 0) & (late < chunks))
            def _(late=late, hop=hop):
                relay(late, hop)
        return carry

    lax.fori_loop(0, chunks + LAG * (nz - 2), body, 0)

    def finish(j, carry):
        t = j * nz + z

        @pl.when(z > 0)
        def _():
            up_copy(t).wait_recv()
            part[t] = part[t] + from_lo[t]

        @pl.when(z < nz - 1)
        def _():
            down_copy(t).wait_recv()
            part[t] = part[t] + from_hi[t]
        out_ref[:, pl.ds(pl.multiple_of(j * CHUNK, CHUNK), CHUNK), :] = part[t]
        return carry

    lax.fori_loop(0, rows, finish, 0)

    for step in range(1, nz):
        rhs_copy(nz - step).wait_recv()
    total = rsum[...]
    for step in range(1, nz):
        total = total + rrecv[step]
    rhs_ref[...] = total

    for step in range(1, nq):
        small_copy(step).wait_send()
    for step in range(1, nz):
        rhs_copy(step).wait_send()

    def drain(t, carry):
        for step in range(1, nq):
            plane_copy(t, step).wait_send()

        @pl.when(lax.rem(t, nz) != z)
        def _():
            up_copy(t).wait_send()
        return carry

    lax.fori_loop(0, chunks, drain, 0)


def spread(nq, nz, schur, small):
    params = schur.shape[0]
    chunks = params // CHUNK
    groups = params // LANES
    block = pltpu.VMEM((chunks, NWIN, CHUNK, LANES), jnp.float32)
    dma = pltpu.SemaphoreType.DMA
    return pl.pallas_call(
        functools.partial(spread_kernel, nq, nz),
        out_shape=(jax.ShapeDtypeStruct((NWIN, params // nz, LANES), jnp.float32),
                   jax.ShapeDtypeStruct((NWIN, groups, LANES), jnp.float32)),
        in_specs=[pl.BlockSpec(memory_space=pl.ANY), pl.BlockSpec(memory_space=pltpu.VMEM)],
        out_specs=(pl.BlockSpec(memory_space=pltpu.VMEM), pl.BlockSpec(memory_space=pltpu.VMEM)),
        scratch_shapes=[
            pltpu.VMEM((nq, chunks, CHUNK, LANES), jnp.float32),
            pltpu.VMEM((nq, 2 * groups, LANES), jnp.float32),
            block, block, block,
            pltpu.VMEM((NWIN, groups, LANES), jnp.float32),
            pltpu.VMEM((nz, NWIN, groups, LANES), jnp.float32),
            dma((chunks,)), dma((nq, chunks)), dma((nq, chunks)), dma((nq,)), dma((nq,)),
            dma((chunks,)), dma((chunks,)), dma((chunks,)), dma((nz,)), dma((nz,)),
        ],
        compiler_params=pltpu.CompilerParams(
            collective_id=0, has_side_effects=True, vmem_limit_bytes=40 * 1024 * 1024),
        name="spread",
    )(schur, small)


def reduced_bundle(local_b, global_b, resid_b, weight_b, count):
    measure_slot, local_param = local_b.shape
    slots = jnp.arange(measure_slot, dtype=jnp.int32)
    live = jnp.where(slots < count, weight_b, jnp.float32(0.0))
    root = jnp.sqrt(live)[:, None]
    ls = local_b * root
    gs = global_b * root
    rs = resid_b[:, None] * root
    curv = tdot(ls, ls) + jnp.eye(local_param, dtype=jnp.float32)
    coupling = tdot(ls, gs)
    lr = tdot(ls, rs)
    gr = tdot(gs, rs)[:, 0]
    factor = jnp.linalg.cholesky(curv)
    solved_all = jax.scipy.linalg.cho_solve((factor, True), jnp.concatenate([coupling, lr], axis=1))
    solved, solved_rhs = solved_all[:, :-1], solved_all[:, -1:]
    schur = tdot(gs, gs, HIGH) - tdot(coupling, solved, HIGH)
    reduced = gr - tdot(coupling, solved_rhs)[:, 0]
    return schur, reduced


def on_device(local_slopes, global_slopes, residuals, weights, track_slot_count, windows):
    nq, nz = lax.axis_size("wide"), lax.axis_size("narrow")
    slots, params = global_slopes.shape[1:]
    owned = params // nz
    z = lax.axis_index("narrow")
    if params // nq == LANES and local_slopes.shape[2] == LANES and owned % CHUNK == 0 and nz > 1:
        schur, small = reduce_bundle(track_slot_count, windows, local_slopes[0], global_slopes[0],
                                     residuals, weights)
        matrix, rhs = spread(nq, nz, schur, small)
        return matrix, lax.dynamic_slice_in_dim(rhs.reshape(NWIN, params), z * owned, owned, 1)
    schur, reduced = reduced_bundle(
        local_slopes[0], global_slopes[0], residuals[0], weights[0], track_slot_count[0])
    picks = (windows[0] == jnp.arange(NWIN, dtype=jnp.int32)).astype(jnp.float32)
    rhs_whole = lax.psum(picks[:, None] * reduced[None], ("wide", "narrow"))
    normal_rhs = lax.dynamic_slice_in_dim(rhs_whole, z * owned, owned, 1)
    received = lax.all_to_all(schur[None], "wide", split_axis=2, concat_axis=0, tiled=True)
    all_picks = lax.all_gather(picks, "wide", axis=0)
    partial_value = jnp.einsum("bw,bij->wij", all_picks, received, precision=HIGHEST,
                               preferred_element_type=jnp.float32)
    return lax.psum_scatter(partial_value, "narrow", scatter_dimension=1, tiled=True), normal_rhs


def solution(mesh):
    in_specs = (
        P(("wide", "narrow"), None, None),
        P(("wide", "narrow"), None, None),
        P(("wide", "narrow"), None),
        P(("wide", "narrow"), None),
        P(("wide", "narrow")),
        P(("wide", "narrow")),
    )
    out_specs = (P(None, "narrow", "wide"), P(None, "narrow"))
    return jax.shard_map(
        on_device, mesh=mesh, in_specs=in_specs, out_specs=out_specs, check_vma=False
    )
```

```python
import functools
import jax
import jax.numpy as jnp
from jax import lax
from jax.experimental import pallas as pl
from jax.experimental.pallas import tpu as pltpu
from jax.sharding import PartitionSpec as P

WINDOW_PARAMS = 1024
NWIN = 4
LANES = 128
CHUNK = 64
AHEAD = 3
LAG = 2
MESH = pl.DeviceIdType.MESH
HIGHEST = lax.Precision.HIGHEST
HIGH = lax.Precision.HIGH


def tdot(left, right, precision=HIGHEST):
    return lax.dot_general(
        left,
        right,
        (((0,), (0,)), ((), ())),
        precision=precision,
        preferred_element_type=jnp.float32,
    )


def invert(c):
    size = c.shape[0]
    sub = lax.broadcasted_iota(jnp.int32, (8, size), 0)
    lane = lax.broadcasted_iota(jnp.int32, (8, size), 1)
    rows = [c[r:r + 8, :] for r in range(0, size, 8)]
    for k in range(0, size, 2):
        r, o = divmod(k, 8)
        left = [jnp.broadcast_to(x[:, k:k + 1], x.shape) for x in rows]
        right = [jnp.broadcast_to(x[:, k + 1:k + 2], x.shape) for x in rows]
        r0 = jnp.broadcast_to(rows[r][o:o + 1, :], (8, size))
        r1 = jnp.broadcast_to(rows[r][o + 1:o + 2, :], (8, size))
        a = jnp.broadcast_to(left[r][o:o + 1, :], (8, size))
        b_low = jnp.broadcast_to(left[r][o + 1:o + 2, :], (8, size))
        b = jnp.broadcast_to(right[r][o:o + 1, :], (8, size))
        d = jnp.broadcast_to(right[r][o + 1:o + 2, :], (8, size))
        inv = 1.0 / (a * d - b * b_low)
        here, after = lane == k, lane == k + 1
        r0 = jnp.where(here, 1.0, jnp.where(after, 0.0, r0))
        r1 = jnp.where(after, 1.0, jnp.where(here, 0.0, r1))
        p0 = (d * r0 - b * r1) * inv
        p1 = (a * r1 - b_low * r0) * inv
        pair = here | after
        rows = [jnp.where(pair, 0.0, x) - u * p0 - v * p1 for x, u, v in zip(rows, left, right)]
        rows[r] = jnp.where(sub == o, p0, jnp.where(sub == o + 1, p1, rows[r]))
    return jnp.concatenate(rows, axis=0)


def split(x):
    high = x.astype(jnp.bfloat16)
    return high, (x - high.astype(jnp.float32)).astype(jnp.bfloat16)


def bundle_kernel(count_ref, window_ref, local_ref, global_ref, resid_ref, weight_ref,
                  schur_ref, small_ref, high, low, u_high, u_low, x_high, x_low, gr):
    slots, params = global_ref.shape
    size = local_ref.shape[1]
    groups = params // LANES
    slot = lax.broadcasted_iota(jnp.int32, (1, slots), 1)
    root = jnp.sqrt(jnp.where(slot < count_ref[0], weight_ref[...], 0.0))
    root_col = jnp.broadcast_to(root, (LANES, slots)).T
    rs_col = jnp.broadcast_to(root * resid_ref[...], (LANES, slots)).T
    ls = local_ref[...] * root_col
    eye = (lax.broadcasted_iota(jnp.int32, (size, size), 0)
           == lax.broadcasted_iota(jnp.int32, (size, size), 1)).astype(jnp.float32)
    ls_t = ls.T
    inverse = invert(jnp.dot(ls_t, ls, precision=HIGHEST, preferred_element_type=jnp.float32) + eye)
    lr = jnp.sum(ls * rs_col, axis=0, keepdims=True)
    lr_col = jnp.broadcast_to(lr, (LANES, size)).T
    for g in range(groups):
        cols = slice(g * LANES, (g + 1) * LANES)
        gs = global_ref[:, cols] * root_col
        high[:, cols], low[:, cols] = split(gs)
        coupling = jnp.dot(ls_t, gs, precision=HIGHEST, preferred_element_type=jnp.float32)
        solved = jnp.dot(inverse, coupling, precision=HIGHEST, preferred_element_type=jnp.float32)
        u_high[:, cols], u_low[:, cols] = split(coupling)
        x_high[:, cols], x_low[:, cols] = split(solved)
        gr[g:g + 1, :] = (jnp.sum(gs * rs_col, axis=0, keepdims=True)
                          - jnp.sum(solved * lr_col, axis=0, keepdims=True))
    small_ref[:groups, :] = gr[...]
    small_ref[groups:, :] = (lax.broadcasted_iota(jnp.int32, (groups, LANES), 0)
                             == window_ref[0]).astype(jnp.float32)

    @pl.loop(0, groups)
    def _(i):
        cols = pl.ds(pl.multiple_of(i * LANES, LANES), LANES)

        def product(left, right):
            return lax.dot_general(left[:, cols], right[...], (((0,), (0,)), ((), ())),
                                   preferred_element_type=jnp.float32)

        gram = product(high, high) + (product(high, low) + product(low, high))
        taken = product(u_high, x_high) + (product(u_high, x_low) + product(u_low, x_high))
        schur_ref[cols, :] = gram - taken


def reduce_bundle(count, window, local_b, global_b, resid, weight):
    slots, params = global_b.shape
    size = local_b.shape[1]
    groups = params // LANES
    smem = pl.BlockSpec(memory_space=pltpu.SMEM)
    vmem = pl.BlockSpec(memory_space=pltpu.VMEM)
    bf16 = jnp.bfloat16
    return pl.pallas_call(
        bundle_kernel,
        out_shape=(jax.ShapeDtypeStruct((params, params), jnp.float32),
                   jax.ShapeDtypeStruct((2 * groups, LANES), jnp.float32)),
        in_specs=[smem, smem, vmem, vmem, vmem, vmem],
        out_specs=(vmem, vmem),
        scratch_shapes=[
            pltpu.VMEM((slots, params), bf16), pltpu.VMEM((slots, params), bf16),
            pltpu.VMEM((size, params), bf16), pltpu.VMEM((size, params), bf16),
            pltpu.VMEM((size, params), bf16), pltpu.VMEM((size, params), bf16),
            pltpu.VMEM((groups, LANES), jnp.float32),
        ],
        compiler_params=pltpu.CompilerParams(vmem_limit_bytes=24 * 1024 * 1024),
        name="bundle",
    )(count, window, local_b, global_b, resid, weight)


def spread_kernel(nq, nz, s_ref, small_ref, out_ref, rhs_ref,
                  recv, small, part, from_lo, from_hi, mirror, rsum, rrecv,
                  own_sem, send_sem, recv_sem, small_send, small_recv,
                  z_send, lo_sem, hi_sem, r_send, r_recv, m_send, m_recv):
    q = lax.axis_index("wide")
    z = lax.axis_index("narrow")
    chunks = recv.shape[1]
    half = nq // 2
    cuts = LANES // CHUNK
    per_z = nq // nz
    groups = small.shape[1] // 2

    def peer(step):
        return lax.rem(q + step, nq)

    barrier = pltpu.get_barrier_semaphore()
    for dz in range(nz):
        for step in range(nq):
            if dz or step:
                pl.semaphore_signal(barrier, inc=1, device_id=(peer(step), lax.rem(z + dz, nz)),
                                    device_id_type=MESH)
    pl.semaphore_wait(barrier, nq * nz - 1)

    def block_of(t, col):
        return lax.rem(col + lax.rem(t, half + 1), nq)

    def target(t):
        return block_of(t, q) // per_z

    def cut_of(t):
        return t // (half + 1)

    def piece(t, col):
        row = block_of(t, col) * LANES + cut_of(t) * CHUNK
        return s_ref.at[pl.ds(pl.multiple_of(row, CHUNK), CHUNK), pl.ds(pl.multiple_of(col * LANES, LANES), LANES)]

    def plane_copy(t, step):
        return pltpu.make_async_remote_copy(
            src_ref=piece(t, peer(step)), dst_ref=recv.at[nq - step, t],
            send_sem=send_sem.at[step, t], recv_sem=recv_sem.at[nq - step, t],
            device_id=(peer(step), z), device_id_type=MESH)

    def own_copy(t):
        return pltpu.make_async_copy(piece(t, q), recv.at[0, t], own_sem.at[t])

    def small_copy(step):
        return pltpu.make_async_remote_copy(
            src_ref=small_ref, dst_ref=small.at[nq - step],
            send_sem=small_send.at[step], recv_sem=small_recv.at[nq - step],
            device_id=(peer(step), z), device_id_type=MESH)

    def up_copy(t):
        return pltpu.make_async_remote_copy(
            src_ref=part.at[t], dst_ref=from_lo.at[t], send_sem=z_send.at[t], recv_sem=lo_sem.at[t],
            device_id=(q, lax.min(z + 1, nz - 1)), device_id_type=MESH)

    def down_copy(t):
        return pltpu.make_async_remote_copy(
            src_ref=part.at[t], dst_ref=from_hi.at[t], send_sem=z_send.at[t], recv_sem=hi_sem.at[t],
            device_id=(q, lax.max(z - 1, 0)), device_id_type=MESH)

    def rhs_copy(step):
        return pltpu.make_async_remote_copy(
            src_ref=rsum, dst_ref=rrecv.at[nz - step],
            send_sem=r_send.at[step], recv_sem=r_recv.at[nz - step],
            device_id=(q, lax.rem(z + step, nz)), device_id_type=MESH)

    def mirror_copy(t):
        d = lax.rem(t, half + 1)
        return pltpu.make_async_remote_copy(
            src_ref=part.at[t], dst_ref=mirror.at[t], send_sem=m_send.at[t], recv_sem=m_recv.at[t],
            device_id=(lax.rem(q + d, nq), q // per_z), device_id_type=MESH)

    order = sorted(range(1, nq), key=lambda step: -min(step, nq - step))

    def send_chunk(t):
        for step in order:
            plane_copy(t, step).start()
        own_copy(t).start()

    for step in order:
        small_copy(step).start()
    for t in range(AHEAD):
        send_chunk(t)
    small[0] = small_ref[...]
    for step in range(1, nq):
        small_copy(nq - step).wait_recv()
    for w in range(NWIN):
        total = jnp.zeros((groups, LANES), jnp.float32)
        for s in range(nq):
            total = total + small[s, groups + w:groups + w + 1, :] * small[s, :groups, :]
        rsum[w] = total
    for step in range(1, nz):
        rhs_copy(step).start()

    def relay(t, hop):
        n = target(t)
        if hop == 0:
            @pl.when((z == 0) & (n > 0))
            def _():
                up_copy(t).start()

            @pl.when((z == nz - 1) & (n < nz - 1))
            def _():
                down_copy(t).start()
        else:
            @pl.when((z == hop) & (n > z))
            def _():
                up_copy(t).wait_recv()
                part[t] = part[t] + from_lo[t]
                up_copy(t).start()

            @pl.when((z == nz - 1 - hop) & (n < z))
            def _():
                down_copy(t).wait_recv()
                part[t] = part[t] + from_hi[t]
                down_copy(t).start()

    def finish(t):
        @pl.when(target(t) == z)
        def _():
            @pl.when(z > 0)
            def _():
                up_copy(t).wait_recv()
                part[t] = part[t] + from_lo[t]

            @pl.when(z < nz - 1)
            def _():
                down_copy(t).wait_recv()
                part[t] = part[t] + from_hi[t]
            d = lax.rem(t, half + 1)

            @pl.when((d > 0) & (d < half))
            def _():
                mirror_copy(t).start()
            row = lax.rem(block_of(t, q), per_z) * LANES + cut_of(t) * CHUNK
            out_ref[:, pl.ds(pl.multiple_of(row, CHUNK), CHUNK), :] = part[t]

    def body(t, carry):
        @pl.when(t + AHEAD < chunks)
        def _():
            send_chunk(t + AHEAD)

        @pl.when(t < chunks)
        def _():
            own_copy(t).wait()
            for step in order:
                plane_copy(t, nq - step).wait_recv()
            for w in range(NWIN):
                total = jnp.zeros((CHUNK, LANES), jnp.float32)
                for s in range(nq):
                    total = total + small[s, groups + w:groups + w + 1, :] * recv[s, t]
                part[t, w] = total
            relay(t, 0)
        for hop in range(1, nz - 1):
            late = t - LAG * hop

            @pl.when((late >= 0) & (late < chunks))
            def _(late=late, hop=hop):
                relay(late, hop)
        last = t - LAG * (nz - 1)

        @pl.when(last >= 0)
        def _():
            finish(last)
        return carry

    lax.fori_loop(0, chunks + LAG * (nz - 1), body, 0)

    for d in range(1, half):
        source = lax.rem(q + nq - d, nq)

        @pl.when(source // per_z == z)
        def _(d=d, source=source):
            for cut in range(cuts):
                mirror_copy(cut * (half + 1) + d).wait_recv()
            row = lax.rem(source, per_z) * LANES
            for w in range(NWIN):
                block = jnp.concatenate([mirror[cut * (half + 1) + d, w] for cut in range(cuts)], axis=0)
                out_ref[w, pl.ds(pl.multiple_of(row, LANES), LANES), :] = block.T

    for step in range(1, nz):
        rhs_copy(nz - step).wait_recv()
    total = rsum[...]
    for step in range(1, nz):
        total = total + rrecv[step]
    rhs_ref[...] = total

    for step in range(1, nq):
        small_copy(step).wait_send()
    for step in range(1, nz):
        rhs_copy(step).wait_send()

    def drain(t, carry):
        for step in range(1, nq):
            plane_copy(t, step).wait_send()
        d = lax.rem(t, half + 1)

        @pl.when(target(t) != z)
        def _():
            up_copy(t).wait_send()

        @pl.when((target(t) == z) & (d > 0) & (d < half))
        def _():
            mirror_copy(t).wait_send()
        return carry

    lax.fori_loop(0, chunks, drain, 0)


def spread(nq, nz, schur, small):
    params = schur.shape[0]
    groups = params // LANES
    chunks = (nq // 2 + 1) * (LANES // CHUNK)
    block = pltpu.VMEM((chunks, NWIN, CHUNK, LANES), jnp.float32)
    dma = pltpu.SemaphoreType.DMA
    return pl.pallas_call(
        functools.partial(spread_kernel, nq, nz),
        out_shape=(jax.ShapeDtypeStruct((NWIN, params // nz, LANES), jnp.float32),
                   jax.ShapeDtypeStruct((NWIN, groups, LANES), jnp.float32)),
        in_specs=[pl.BlockSpec(memory_space=pl.ANY), pl.BlockSpec(memory_space=pltpu.VMEM)],
        out_specs=(pl.BlockSpec(memory_space=pltpu.VMEM), pl.BlockSpec(memory_space=pltpu.VMEM)),
        scratch_shapes=[
            pltpu.VMEM((nq, chunks, CHUNK, LANES), jnp.float32),
            pltpu.VMEM((nq, 2 * groups, LANES), jnp.float32),
            block, block, block, block,
            pltpu.VMEM((NWIN, groups, LANES), jnp.float32),
            pltpu.VMEM((nz, NWIN, groups, LANES), jnp.float32),
            dma((chunks,)), dma((nq, chunks)), dma((nq, chunks)), dma((nq,)), dma((nq,)),
            dma((chunks,)), dma((chunks,)), dma((chunks,)), dma((nz,)), dma((nz,)),
            dma((chunks,)), dma((chunks,)),
        ],
        compiler_params=pltpu.CompilerParams(
            collective_id=0, has_side_effects=True, vmem_limit_bytes=40 * 1024 * 1024),
        name="spread",
    )(schur, small)


def reduced_bundle(local_b, global_b, resid_b, weight_b, count):
    measure_slot, local_param = local_b.shape
    slots = jnp.arange(measure_slot, dtype=jnp.int32)
    live = jnp.where(slots < count, weight_b, jnp.float32(0.0))
    root = jnp.sqrt(live)[:, None]
    ls = local_b * root
    gs = global_b * root
    rs = resid_b[:, None] * root
    curv = tdot(ls, ls) + jnp.eye(local_param, dtype=jnp.float32)
    coupling = tdot(ls, gs)
    lr = tdot(ls, rs)
    gr = tdot(gs, rs)[:, 0]
    factor = jnp.linalg.cholesky(curv)
    solved_all = jax.scipy.linalg.cho_solve((factor, True), jnp.concatenate([coupling, lr], axis=1))
    solved, solved_rhs = solved_all[:, :-1], solved_all[:, -1:]
    schur = tdot(gs, gs, HIGH) - tdot(coupling, solved, HIGH)
    reduced = gr - tdot(coupling, solved_rhs)[:, 0]
    return schur, reduced


def on_device(local_slopes, global_slopes, residuals, weights, track_slot_count, windows):
    nq, nz = lax.axis_size("wide"), lax.axis_size("narrow")
    slots, params = global_slopes.shape[1:]
    owned = params // nz
    z = lax.axis_index("narrow")
    if params // nq == LANES and local_slopes.shape[2] == LANES and owned % LANES == 0 and nq % 2 == 0 and nz > 1:
        schur, small = reduce_bundle(track_slot_count, windows, local_slopes[0], global_slopes[0],
                                     residuals, weights)
        matrix, rhs = spread(nq, nz, schur, small)
        return matrix, lax.dynamic_slice_in_dim(rhs.reshape(NWIN, params), z * owned, owned, 1)
    schur, reduced = reduced_bundle(
        local_slopes[0], global_slopes[0], residuals[0], weights[0], track_slot_count[0])
    picks = (windows[0] == jnp.arange(NWIN, dtype=jnp.int32)).astype(jnp.float32)
    rhs_whole = lax.psum(picks[:, None] * reduced[None], ("wide", "narrow"))
    normal_rhs = lax.dynamic_slice_in_dim(rhs_whole, z * owned, owned, 1)
    received = lax.all_to_all(schur[None], "wide", split_axis=2, concat_axis=0, tiled=True)
    all_picks = lax.all_gather(picks, "wide", axis=0)
    partial_value = jnp.einsum("bw,bij->wij", all_picks, received, precision=HIGHEST,
                               preferred_element_type=jnp.float32)
    return lax.psum_scatter(partial_value, "narrow", scatter_dimension=1, tiled=True), normal_rhs


def solution(mesh):
    in_specs = (
        P(("wide", "narrow"), None, None),
        P(("wide", "narrow"), None, None),
        P(("wide", "narrow"), None),
        P(("wide", "narrow"), None),
        P(("wide", "narrow")),
        P(("wide", "narrow")),
    )
    out_specs = (P(None, "narrow", "wide"), P(None, "narrow"))
    return jax.shard_map(
        on_device, mesh=mesh, in_specs=in_specs, out_specs=out_specs, check_vma=False
    )
```
